32 devices in a mesh: blocks: 16 (over z, y, x), cross: 2 (over core).
Axes of the slice: x: 2, y: 2, z: 4, core: 2. Of those that a mesh axis runs over, the one named last changes fastest.
Arguments:
- f_home: float32 [1024, 19, 512], P(('blocks', 'cross')), may hold values from -0.5 to 1.5
- levels: int32 [1024], P(('blocks', 'cross')), may hold values from 0 to 1, as said below
- plan: int32 [1024], P(('blocks', 'cross')), may hold values from 0 to 1023, as said below
Outputs:
- f_owner: float32 [1024, 19, 512], P(('blocks', 'cross'))
The draws below stay inside these ranges and needn't reach their ends.
Inputs may be any that keep to these rules, and one draw needn't show every extreme that they name: `levels`: exactly a quarter of the patches, 8 times the number of devices, have level 1. plan is a permutation of the patch numbers. Of the patches in the slots of one device of f_home, at most 2 have owner slots on one device, and in every draw some device sends exactly 2 to one owner; every device's owner slots receive exactly 8 patches of level 1.
All inputs are finite; a program needn't handle non-finite values.
Results may differ from the reference program's by a relative error of at most 0.0001.
Values sent between devices are 32-bit elements; how exact they have to be, the bound alone decides.
No kernel may reach another device: no remote copies, remote signals or barrier semaphores. Data moves between devices by JAX's collectives and lax.ppermute only.
A program may use at most 256 MiB of HBM per device.

```python
import jax
import jax.numpy as jnp
from jax import lax

FLOW_PATCHES = 1
SPAN_PATCHES = 4
DEPTH_PATCHES = 8
EDGE = 8
STEPS = 2
CELLS = 512
PATCH_DEV = 32
FINE_DEV = 8
PATCHES = 1024
N_BLOCKS = 16
N_CROSS = 2
DEVICES = 32


VELOCITIES = ((0, 0, 0), (1, 0, 0), (-1, 0, 0), (0, 1, 0), (0, -1, 0), (0, 0, 1), (0, 0, -1), (1, 1, 0), (-1, -1, 0), (1, -1, 0), (-1, 1, 0), (1, 0, 1), (-1, 0, -1), (1, 0, -1), (-1, 0, 1), (0, 1, 1), (0, -1, -1), (0, 1, -1), (0, -1, 1))


WEIGHTS = (1.0 / 3.0,) + (1.0 / 18.0,) * 6 + (1.0 / 36.0,) * 12


def wake_layout(key):
    key_tie = jax.random.fold_in(key, 7)
    key_owner = jax.random.fold_in(key, 8)
    key_slot = jax.random.fold_in(key, 9)
    key_jitter = jax.random.fold_in(key, 10)
    ident = jnp.arange(PATCHES, dtype=jnp.int32)
    home = ident // PATCH_DEV
    local_id = ident % PATCH_DEV
    flow_x = home // N_CROSS * FLOW_PATCHES + local_id // (SPAN_PATCHES * DEPTH_PATCHES)
    span_y = home % N_CROSS * SPAN_PATCHES + local_id // DEPTH_PATCHES % SPAN_PATCHES
    total_x = FLOW_PATCHES * N_BLOCKS
    total_y = SPAN_PATCHES * N_CROSS
    behind = flow_x - total_x // 8
    lateral = jnp.abs(2 * span_y + 1 - total_y)
    jitter = jax.random.randint(key_jitter, (PATCHES,), 0, 3 * total_x)
    score = jnp.where(behind >= 0, 8 * total_x * total_y, 0) - lateral * total_x - jnp.abs(behind - total_x // 4) * total_y + jitter
    ties = jax.random.permutation(key_tie, PATCHES).astype(jnp.int32)
    order = jnp.argsort(-(score * PATCHES + ties))
    fine_mask = jnp.zeros((PATCHES,), jnp.int32).at[order[:PATCHES // 4]].set(1)
    fine_rank = jnp.cumsum(fine_mask) - 1
    coarse_rank = jnp.cumsum(1 - fine_mask) - 1
    home_fine = jnp.sum(fine_mask.reshape(DEVICES, PATCH_DEV), axis=1)
    home_coarse = PATCH_DEV - home_fine
    fine_before = jnp.cumsum(home_fine) - home_fine
    coarse_before = jnp.arange(DEVICES, dtype=jnp.int32) * PATCH_DEV - fine_before
    chosen = jnp.argmax(jnp.where(home_coarse > 0, home_fine, -1))
    offset = (fine_before[chosen] - coarse_before[chosen] - home_coarse[chosen] + 1) % DEVICES
    coarse_total = PATCHES - PATCHES // 4
    coarse_index = (coarse_rank + offset) % coarse_total
    owner_pos = jnp.where(fine_mask == 1, fine_rank % DEVICES, coarse_index % DEVICES)
    slot_rank = jnp.where(fine_mask == 1, fine_rank // DEVICES, FINE_DEV + coarse_index // DEVICES)
    relabel = jax.random.permutation(key_owner, DEVICES).astype(jnp.int32)
    slot_scores = jax.random.randint(key_slot, (DEVICES, PATCH_DEV), 0, 1 << 20) * PATCH_DEV + jnp.arange(PATCH_DEV, dtype=jnp.int32)[None, :]
    shuffle = jnp.argsort(slot_scores, axis=1).astype(jnp.int32)
    plan = relabel[owner_pos] * PATCH_DEV + shuffle[owner_pos, slot_rank]
    return (fine_mask.astype(jnp.int32), plan.astype(jnp.int32))


def draw_levels(key, part):
    return wake_layout(key)[0]


def draw_plan(key, part):
    return wake_layout(key)[1]


def draw_f_home(key, part):
    key_density = jax.random.fold_in(key, 21)
    key_velocity = jax.random.fold_in(key, 22)
    key_jitter = jax.random.fold_in(key, 23)
    density = 1.0 + 0.05 * jax.random.truncated_normal(key_density, -3.0, 3.0, (PATCHES, CELLS), jnp.float32)
    velocity = 0.03 * jax.random.truncated_normal(key_velocity, -3.0, 3.0, (3, PATCHES, CELLS), jnp.float32)
    velocity = velocity.at[0].add(0.05)
    jitter = jax.random.truncated_normal(key_jitter, -3.0, 3.0, (PATCHES, 19, CELLS), jnp.float32)
    speed_sq = velocity[0] * velocity[0] + velocity[1] * velocity[1] + velocity[2] * velocity[2]
    columns = []
    for speed in range(19):
        step_x, step_y, step_z = VELOCITIES[speed]
        along = step_x * velocity[0] + step_y * velocity[1] + step_z * velocity[2]
        columns.append(WEIGHTS[speed] * (density * (1.0 + 3.0 * along + 4.5 * along * along - 1.5 * speed_sq) + 0.3 * jitter[:, speed]))
    return jnp.stack(columns, axis=1).astype(jnp.float32)


def block_scale(rng, shape, split, low, top_value):
    loudness = 1.0
    for dim, shards_of in split:
        steps = jax.random.uniform(jax.random.fold_in(jax.random.fold_in(rng, 6), dim), (shards_of,), jnp.float32, low / len(split), top_value / len(split))
        loudness = loudness * jnp.repeat(jnp.exp(steps), shape[dim] // shards_of).reshape((-1,) + (1,) * (len(shape) - 1 - dim))
    return loudness


def setup_inputs(seed: int = 0) -> dict:
    seeds = jax.random.split(jax.random.key(seed), 4)
    f_home = draw_f_home(jax.random.fold_in(seeds[3], 71), 0)
    levels = draw_levels(jax.random.fold_in(seeds[3], 71), 0)
    plan = draw_plan(jax.random.fold_in(seeds[3], 71), 0)
    return dict(f_home=f_home, levels=levels, plan=plan)


VELOCITIES = ((0, 0, 0), (1, 0, 0), (-1, 0, 0), (0, 1, 0), (0, -1, 0), (0, 0, 1), (0, 0, -1), (1, 1, 0), (-1, -1, 0), (1, -1, 0), (-1, 1, 0), (1, 0, 1), (-1, 0, -1), (1, 0, -1), (-1, 0, 1), (0, 1, 1), (0, -1, -1), (0, 1, -1), (0, -1, 1))
WEIGHTS = (1.0 / 3.0,) + (1.0 / 18.0,) * 6 + (1.0 / 36.0,) * 12
FACE_SPEEDS = ((2, 8, 10, 12, 14), (1, 7, 9, 11, 13), (4, 8, 9, 16, 18), (3, 7, 10, 15, 17), (6, 12, 13, 16, 17), (5, 11, 14, 15, 18))
TAU_COARSE = 0.55
TAU_FINE = 2.0 * TAU_COARSE - 0.5
RESCALE = TAU_FINE / (2.0 * TAU_COARSE)
INFLOW = 0.08


def moments(field):
    density = jnp.sum(field, axis=1)
    velocity = []
    for axis_id in range(3):
        forward = [speed for speed in range(19) if VELOCITIES[speed][axis_id] == 1]
        backward = [speed for speed in range(19) if VELOCITIES[speed][axis_id] == -1]
        velocity.append((jnp.sum(field[:, forward], axis=1) - jnp.sum(field[:, backward], axis=1)) / density)
    return density, velocity


def equilibrium(density, velocity, speeds):
    speed_sq = velocity[0] * velocity[0] + velocity[1] * velocity[1] + velocity[2] * velocity[2]
    columns = []
    for speed in speeds:
        step_x, step_y, step_z = VELOCITIES[speed]
        along = step_x * velocity[0] + step_y * velocity[1] + step_z * velocity[2]
        columns.append(WEIGHTS[speed] * density * (1.0 + 3.0 * along + 4.5 * along * along - 1.5 * speed_sq))
    return jnp.stack(columns, axis=1)


def collide(field, relax_rate):
    density, velocity = moments(field)
    balance = equilibrium(density, velocity, range(19))
    relaxed = field + relax_rate[:, None, None, None, None] * (balance - field)
    return relaxed, balance, density, velocity


def layer(field, face_id):
    layer_at = 0 if face_id % 2 == 0 else field.shape[-1] - 1
    return jnp.take(field, layer_at, axis=2 + face_id // 2)


def face_payload(relaxed, balance, send_scale):
    eq_faces = jnp.stack([layer(balance[:, list(FACE_SPEEDS[face_id])], face_id) for face_id in range(6)], axis=1)
    out_faces = jnp.stack([layer(relaxed[:, list(FACE_SPEEDS[face_id])], face_id) for face_id in range(6)], axis=1)
    return eq_faces, send_scale[:, None, None, None, None] * (out_faces - eq_faces)


def inflow_column(speeds):
    values = []
    for speed in speeds:
        along = VELOCITIES[speed][0] * INFLOW
        values.append(WEIGHTS[speed] * (1.0 + 3.0 * along + 4.5 * along * along - 1.5 * INFLOW * INFLOW))
    return jnp.array(values, jnp.float32)


def framed(center, top_row, bottom_row, left_col, right_col):
    middle = jnp.concatenate([left_col[..., :, None], center, right_col[..., :, None]], axis=-1)
    corner = jnp.zeros(top_row.shape[:-1] + (1,), top_row.dtype)
    upper = jnp.concatenate([corner, top_row, corner], axis=-1)[..., None, :]
    lower = jnp.concatenate([corner, bottom_row, corner], axis=-1)[..., None, :]
    return jnp.concatenate([upper, middle, lower], axis=-2)


def bordered(center, left_col, right_col):
    return jnp.concatenate([left_col[..., None], center, right_col[..., None]], axis=-1)


def assemble(eq_ext, neq_ext, recv_scale, inflow_side, outflow_side):
    size_x, size_y, size_z = recv_scale.shape
    factor = recv_scale[:, :, :, None, None, None]

    def neighbour(shift_x, shift_y, shift_z, face_id):
        window = (slice(1 + shift_x, 1 + shift_x + size_x), slice(1 + shift_y, 1 + shift_y + size_y), slice(1 + shift_z, 1 + shift_z + size_z), face_id)
        return eq_ext[window] + factor * neq_ext[window]

    plane_west = framed(neighbour(-1, 0, 0, 1), neighbour(-1, -1, 0, 1)[..., -1, :], neighbour(-1, 1, 0, 1)[..., 0, :], neighbour(-1, 0, -1, 1)[..., :, -1], neighbour(-1, 0, 1, 1)[..., :, 0])
    plane_east = framed(neighbour(1, 0, 0, 0), neighbour(1, -1, 0, 0)[..., -1, :], neighbour(1, 1, 0, 0)[..., 0, :], neighbour(1, 0, -1, 0)[..., :, -1], neighbour(1, 0, 1, 0)[..., :, 0])
    plane_south = bordered(neighbour(0, -1, 0, 3), neighbour(0, -1, -1, 3)[..., :, -1], neighbour(0, -1, 1, 3)[..., :, 0])
    plane_north = bordered(neighbour(0, 1, 0, 2), neighbour(0, 1, -1, 2)[..., :, -1], neighbour(0, 1, 1, 2)[..., :, 0])
    plane_below = neighbour(0, 0, -1, 5)
    plane_above = neighbour(0, 0, 1, 4)
    plane_west = jnp.where(inflow_side[:, None, None, None, None, None], inflow_column(FACE_SPEEDS[1])[:, None, None], plane_west)
    plane_east = jnp.where(outflow_side[:, None, None, None, None, None], inflow_column(FACE_SPEEDS[0])[:, None, None], plane_east)
    return plane_west, plane_east, plane_south, plane_north, plane_below, plane_above


def propagate(relaxed, planes):
    patch_total = relaxed.shape[0]
    extent = relaxed.shape[-1]
    padded = jnp.zeros((patch_total, 19, extent + 2, extent + 2, extent + 2), relaxed.dtype)
    padded = padded.at[:, :, 1:extent + 1, 1:extent + 1, 1:extent + 1].set(relaxed)
    plane_west, plane_east, plane_south, plane_north, plane_below, plane_above = planes
    for column, speed in enumerate(FACE_SPEEDS[1]):
        padded = padded.at[:, speed, 0, :, :].set(plane_west[:, column])
    for column, speed in enumerate(FACE_SPEEDS[0]):
        padded = padded.at[:, speed, extent + 1, :, :].set(plane_east[:, column])
    for column, speed in enumerate(FACE_SPEEDS[3]):
        padded = padded.at[:, speed, 1:extent + 1, 0, :].set(plane_south[:, column])
    for column, speed in enumerate(FACE_SPEEDS[2]):
        padded = padded.at[:, speed, 1:extent + 1, extent + 1, :].set(plane_north[:, column])
    for column, speed in enumerate(FACE_SPEEDS[5]):
        padded = padded.at[:, speed, 1:extent + 1, 1:extent + 1, 0].set(plane_below[:, column])
    for column, speed in enumerate(FACE_SPEEDS[4]):
        padded = padded.at[:, speed, 1:extent + 1, 1:extent + 1, extent + 1].set(plane_above[:, column])
    shifted = []
    for speed in range(19):
        step_x, step_y, step_z = VELOCITIES[speed]
        shifted.append(padded[:, speed, 1 - step_x:1 - step_x + extent, 1 - step_y:1 - step_y + extent, 1 - step_z:1 - step_z + extent])
    return jnp.stack(shifted, axis=1)


def lattice_order(values):
    trailing = values.shape[1:]
    lattice = values.reshape((N_BLOCKS, N_CROSS, FLOW_PATCHES, SPAN_PATCHES, DEPTH_PATCHES) + trailing)
    lattice = jnp.moveaxis(lattice, 2, 1)
    return lattice.reshape((N_BLOCKS * FLOW_PATCHES, N_CROSS * SPAN_PATCHES, DEPTH_PATCHES) + trailing)


def id_order(lattice):
    trailing = lattice.shape[3:]
    grouped = lattice.reshape((N_BLOCKS, FLOW_PATCHES, N_CROSS, SPAN_PATCHES, DEPTH_PATCHES) + trailing)
    grouped = jnp.moveaxis(grouped, 1, 2)
    return grouped.reshape((PATCHES,) + trailing)


def wrap_axis(values, axis_id):
    length = values.shape[axis_id]
    return jnp.concatenate([lax.slice_in_dim(values, length - 1, length, axis=axis_id), values, lax.slice_in_dim(values, 0, 1, axis=axis_id)], axis=axis_id)


def grouped(values):
    return values.reshape((N_BLOCKS * N_CROSS, PATCH_DEV) + values.shape[1:])


def reference(f_home, levels, plan):
    populations = f_home.reshape(PATCHES, 19, EDGE, EDGE, EDGE)
    fine_mask = levels == 1
    relax_rate = jnp.where(fine_mask, 1.0 / TAU_FINE, 1.0 / TAU_COARSE).astype(jnp.float32)
    send_scale = jnp.where(fine_mask, 1.0 / RESCALE, 1.0).astype(jnp.float32)
    recv_scale = lattice_order(jnp.where(fine_mask, RESCALE, 1.0).astype(jnp.float32))
    span_x = FLOW_PATCHES * N_BLOCKS
    position = jnp.arange(span_x, dtype=jnp.int32)

    def group_faces(pieces):
        relaxed, balance, density, velocity = collide(pieces[0], pieces[1])
        return face_payload(relaxed, balance, pieces[2])

    def group_step(pieces):
        fine_rate = jnp.full((PATCH_DEV,), 1.0 / TAU_FINE, jnp.float32)
        planes = pieces[3:]
        relaxed = collide(pieces[0], pieces[1])[0]
        moved = propagate(relaxed, planes)
        updated = propagate(collide(moved, fine_rate)[0], planes)
        return jnp.where(pieces[2][:, None, None, None, None], updated, moved)

    for round_id in range(STEPS):
        eq_faces, neq_faces = lax.map(group_faces, (grouped(populations), grouped(relax_rate), grouped(send_scale)))
        eq_ext = lattice_order(eq_faces.reshape((PATCHES,) + eq_faces.shape[2:]))
        neq_ext = lattice_order(neq_faces.reshape((PATCHES,) + neq_faces.shape[2:]))
        for axis_id in range(3):
            eq_ext = wrap_axis(eq_ext, axis_id)
            neq_ext = wrap_axis(neq_ext, axis_id)
        planes = assemble(eq_ext, neq_ext, recv_scale, position == 0, position == span_x - 1)
        planes = tuple(grouped(id_order(plane)) for plane in planes)
        populations = lax.map(group_step, (grouped(populations), grouped(relax_rate), grouped(fine_mask)) + planes)
        populations = populations.reshape(PATCHES, 19, EDGE, EDGE, EDGE)
    flattened = populations.reshape(PATCHES, 19, CELLS)
    return jnp.zeros_like(flattened).at[plan].set(flattened)
```

```python
import functools

import jax
import jax.numpy as jnp
from jax import lax
from jax.experimental import pallas as pl
from jax.experimental.pallas import tpu as pltpu
from jax.sharding import PartitionSpec as P

SPAN_PATCHES = 4
DEPTH_PATCHES = 8
EDGE = 8
STEPS = 2
CELLS = 512
LANES = 128
TILES = CELLS // LANES
ROWS = 80

VELOCITIES = (
    (0, 0, 0),
    (1, 0, 0),
    (-1, 0, 0),
    (0, 1, 0),
    (0, -1, 0),
    (0, 0, 1),
    (0, 0, -1),
    (1, 1, 0),
    (-1, -1, 0),
    (1, -1, 0),
    (-1, 1, 0),
    (1, 0, 1),
    (-1, 0, -1),
    (1, 0, -1),
    (-1, 0, 1),
    (0, 1, 1),
    (0, -1, -1),
    (0, 1, -1),
    (0, -1, 1),
)
SPEEDS = 19
WEIGHTS = (1.0 / 3.0,) + (1.0 / 18.0,) * 6 + (1.0 / 36.0,) * 12
EAST = (1, 7, 9, 11, 13)
WEST = (2, 8, 10, 12, 14)
NORTH = (3, 7, 10, 15, 17)
SOUTH = (4, 8, 9, 16, 18)
X_SPEEDS = EAST + WEST
Y_SPEEDS = NORTH + SOUTH
Y_PACKS = 3
DIAG_EAST = ((7, SPAN_PATCHES - 1), (9, 0))
DIAG_WEST = ((10, SPAN_PATCHES - 1), (8, 0))
TAU_COARSE = 0.55
TAU_FINE = 2.0 * TAU_COARSE - 0.5
RESCALE = TAU_FINE / (2.0 * TAU_COARSE)
INFLOW = 0.08


def inflow_value(speed):
    along = VELOCITIES[speed][0] * INFLOW
    return WEIGHTS[speed] * (1.0 + 3.0 * along + 4.5 * along * along - 1.5 * INFLOW * INFLOW)


def lane_roll(tile, shift):
    shift %= LANES
    return tile if shift == 0 else pltpu.roll(tile, shift, 1)


def equilibria(field):
    density = functools.reduce(lambda a, b: a + b, field)
    inverse = 1.0 / density
    velocity = []
    for axis_id in range(3):
        forward = [field[q] for q in range(SPEEDS) if VELOCITIES[q][axis_id] == 1]
        backward = [field[q] for q in range(SPEEDS) if VELOCITIES[q][axis_id] == -1]
        terms = [a - b for a, b in zip(forward, backward)]
        velocity.append(functools.reduce(lambda a, b: a + b, terms) * inverse)
    common = 1.0 - 1.5 * (
        velocity[0] * velocity[0] + velocity[1] * velocity[1] + velocity[2] * velocity[2]
    )
    scaled = {weight: weight * density for weight in set(WEIGHTS)}
    balance = [scaled[WEIGHTS[0]] * common]
    for q in range(1, SPEEDS, 2):
        along = None
        for component, speed in zip(VELOCITIES[q], velocity):
            if component == 0:
                continue
            if along is None:
                along = speed if component == 1 else -speed
            else:
                along = along + speed if component == 1 else along - speed
        even = common + 4.5 * (along * along)
        odd = 3.0 * along
        balance.append(scaled[WEIGHTS[q]] * (even + odd))
        balance.append(scaled[WEIGHTS[q]] * (even - odd))
    return balance


class Masks:
    def __init__(self):
        lane = lax.broadcasted_iota(jnp.int32, (8, LANES), 1)
        self.low = lane < 64
        self.high = lane >= 64
        span = (lane // 8) % 8
        depth = lane % 8
        self.span = span
        self.span_first = span == 0
        self.span_last = span == 7
        self.depth_first = depth == 0
        self.depth_last = depth == 7

    def leaving(self, speed, tile):
        step_x, step_y, step_z = VELOCITIES[speed]
        across_x = None
        if step_x == 1 and tile == TILES - 1:
            across_x = self.high
        if step_x == -1 and tile == 0:
            across_x = self.low
        across_y = {0: None, 1: self.span_last, -1: self.span_first}[step_y]
        across_z = {0: None, 1: self.depth_last, -1: self.depth_first}[step_z]
        return across_x, across_y, across_z

    def leaving_any(self, speed, tile):
        parts = [mask for mask in self.leaving(speed, tile) if mask is not None]
        return functools.reduce(jnp.logical_or, parts) if parts else None

    def shifted(self, tiles, speed):
        step_x, step_y, step_z = VELOCITIES[speed]
        if step_z:
            edge = self.depth_first if step_z == 1 else self.depth_last
            tiles = [
                jnp.where(edge, lane_roll(v, -7 * step_z), lane_roll(v, step_z)) for v in tiles
            ]
        if step_y:
            edge = self.span_first if step_y == 1 else self.span_last
            tiles = [
                jnp.where(edge, lane_roll(v, -56 * step_y), lane_roll(v, 8 * step_y)) for v in tiles
            ]
        if step_x:
            halves = [lane_roll(v, 64) for v in tiles]
            if step_x == 1:
                tiles = [
                    jnp.where(self.low, halves[t - 1], halves[t]) for t in range(TILES)
                ]
            else:
                tiles = [
                    jnp.where(self.low, halves[t], halves[(t + 1) % TILES]) for t in range(TILES)
                ]
        return tiles


def lanes_of(tile):
    return pl.ds(tile * LANES, LANES)


def emit_halos(masks, eq, neq, base, east_ref, west_ref, span_ref, diag_east_ref, diag_west_ref):
    last = TILES - 1

    def east_pack(speed, row):
        e = eq[speed, base + row, :, lanes_of(last)]
        n = neq[speed, base + row, :, lanes_of(last)]
        return jnp.where(masks.low, lane_roll(e, 64), n)

    def west_pack(speed, row):
        e = eq[speed, base + row, :, lanes_of(0)]
        n = neq[speed, base + row, :, lanes_of(0)]
        return jnp.where(masks.low, e, lane_roll(n, 64))

    for column in range(5):
        for row in range(SPAN_PATCHES):
            east_ref[column, row] = east_pack(EAST[column], row)
            west_ref[column, row] = west_pack(WEST[column], row)
    for column, (speed, row) in enumerate(DIAG_EAST):
        diag_east_ref[column] = east_pack(speed, row)
    for column, (speed, row) in enumerate(DIAG_WEST):
        diag_west_ref[column] = west_pack(speed, row)
    for pack_id in range(Y_PACKS):
        for tile in range(TILES):
            packed = jnp.zeros((8, LANES), jnp.float32)
            for slot in range(4):
                index = pack_id * 4 + slot
                if index >= len(Y_SPEEDS):
                    continue
                north = index < 5
                row = base + (SPAN_PATCHES - 1 if north else 0)
                at = 7 if north else 0
                e = eq[Y_SPEEDS[index], row, :, lanes_of(tile)]
                n = neq[Y_SPEEDS[index], row, :, lanes_of(tile)]
                packed = jnp.where(
                    masks.span == 2 * slot, lane_roll(e, 8 * (2 * slot - at)), packed
                )
                packed = jnp.where(
                    masks.span == 2 * slot + 1, lane_roll(n, 8 * (2 * slot + 1 - at)), packed
                )
            span_ref[pack_id, :, lanes_of(tile)] = packed


def take_halos(masks, ends, eq, neq, side_eq, side_neq, east, west, north, south, de, dw):
    for column, speed in enumerate(X_SPEEDS):
        rightward = column < 5
        closed = ends[0 if rightward else 1] == 1
        source, diag, pairs = (east, de, DIAG_EAST) if rightward else (west, dw, DIAG_WEST)
        parts = [(source[column % 5, row], row + 1) for row in range(SPAN_PATCHES)]
        for entry, (diag_speed, row) in enumerate(pairs):
            if diag_speed == speed:
                parts.append((diag[entry], 0 if row else SPAN_PATCHES + 1))
        for packed, row in parts:
            other = lane_roll(packed, 64)
            e, n = (other, packed) if rightward else (packed, other)
            side_eq[column, row] = jnp.where(closed, inflow_value(speed), e)
            side_neq[column, row] = jnp.where(closed, 0.0, n)
    for index, speed in enumerate(Y_SPEEDS):
        from_south = index < 5
        source = north if from_south else south
        row = 0 if from_south else SPAN_PATCHES + 1
        at = 7 if from_south else 0
        slot = index % 4
        for tile in range(TILES):
            packed = source[index // 4, :, lanes_of(tile)]
            eq[speed, row, :, lanes_of(tile)] = lane_roll(packed, 8 * (at - 2 * slot))
            neq[speed, row, :, lanes_of(tile)] = lane_roll(packed, 8 * (at - 2 * slot - 1))


def rates(fine):
    return jnp.where(fine, 1.0 / TAU_FINE, 1.0 / TAU_COARSE)


def open_kernel(level_ref, field_ref, moved_ref, east, west, span, de, dw, eq, neq):
    masks = Masks()

    def row_step(row, carry):
        fine = level_ref[row] == 1
        rate = rates(fine)
        send = jnp.where(fine, 1.0 / RESCALE, 1.0)
        for tile in range(TILES):
            field = []
            for q in range(SPEEDS):
                field.append(field_ref[pl.ds(row * 8, 8), q, lanes_of(tile)])
                moved_ref[q, row, :, lanes_of(tile)] = field[q]
            balance = equilibria(field)
            for q in range(1, SPEEDS):
                relaxed = field[q] + rate * (balance[q] - field[q])
                eq[q, row, :, lanes_of(tile)] = balance[q]
                neq[q, row, :, lanes_of(tile)] = send * (relaxed - balance[q])
        return carry

    lax.fori_loop(0, SPAN_PATCHES, row_step, 0)
    emit_halos(masks, eq, neq, 0, east, west, span, de, dw)


def step_kernel(final, *refs):
    ends, level_ref, field_ref, east, west, north, south, de, dw = refs[:9]
    if final:
        targets, moved_ref = refs[9], refs[10]
        eq, neq, relaxed_ref, side_eq, side_neq, ghost, fresh, again, rows_ref, sems = refs[11:]
    else:
        moved_ref, east_out, west_out, span_out, de_out, dw_out = refs[9:15]
        eq, neq, relaxed_ref, side_eq, side_neq, ghost, fresh, again, eq_next, neq_next = refs[15:]
    masks = Masks()
    take_halos(masks, ends, eq, neq, side_eq, side_neq, east, west, north, south, de, dw)

    def collide_row(row, carry):
        fine = level_ref[row] == 1
        rate = rates(fine)
        send = jnp.where(fine, 1.0 / RESCALE, 1.0)
        for tile in range(TILES):
            field = [field_ref[q, row, :, lanes_of(tile)] for q in range(SPEEDS)]
            balance = equilibria(field)
            for q in range(SPEEDS):
                relaxed = field[q] + rate * (balance[q] - field[q])
                relaxed_ref[q, row, :, lanes_of(tile)] = relaxed
                if q:
                    eq[q, row + 1, :, lanes_of(tile)] = balance[q]
                    neq[q, row + 1, :, lanes_of(tile)] = send * (relaxed - balance[q])
        return carry

    lax.fori_loop(0, SPAN_PATCHES, collide_row, 0)

    def move_row(row, carry):
        fine = level_ref[row] == 1
        scale = jnp.where(fine, RESCALE, 1.0)
        for q in range(SPEEDS):
            _, step_y, step_z = VELOCITIES[q]
            tiles = []
            for tile in range(TILES):
                value = relaxed_ref[q, row, :, lanes_of(tile)]
                across_x, across_y, across_z = masks.leaving(q, tile)

                def source(inner, side, at):
                    picked = inner[q, at, :, lanes_of(tile)]
                    if across_x is not None:
                        picked = jnp.where(across_x, side[X_SPEEDS.index(q), at], picked)
                    return picked

                crossing = masks.leaving_any(q, tile)
                if crossing is not None:
                    pair = []
                    for inner, side in ((eq, side_eq), (neq, side_neq)):
                        picked = source(inner, side, row + 1)
                        if across_y is not None:
                            picked = jnp.where(across_y, source(inner, side, row + 1 - step_y), picked)
                        if across_z is not None:
                            turned = pltpu.roll(picked, step_z % DEPTH_PATCHES, 0)
                            picked = jnp.where(across_z, turned, picked)
                        pair.append(picked)
                    value = jnp.where(crossing, pair[0] + scale * pair[1], value)
                    ghost[q, :, lanes_of(tile)] = value
                tiles.append(value)
            for tile, value in enumerate(masks.shifted(tiles, q)):
                fresh[q, :, lanes_of(tile)] = value
        for tile in range(TILES):
            field = [fresh[q, :, lanes_of(tile)] for q in range(SPEEDS)]
            balance = equilibria(field)
            for q in range(SPEEDS):
                again[q, :, lanes_of(tile)] = field[q] + (1.0 / TAU_FINE) * (balance[q] - field[q])
        for q in range(SPEEDS):
            tiles = []
            for tile in range(TILES):
                value = again[q, :, lanes_of(tile)]
                crossing = masks.leaving_any(q, tile)
                if crossing is not None:
                    value = jnp.where(crossing, ghost[q, :, lanes_of(tile)], value)
                tiles.append(value)
            for tile, value in enumerate(masks.shifted(tiles, q)):
                value = jnp.where(fine, value, fresh[q, :, lanes_of(tile)])
                if final:
                    start = row * (8 * ROWS) + (q * TILES + tile)
                    rows_ref[pl.ds(start, 8, stride=ROWS), :] = value
                else:
                    moved_ref[q, row, :, lanes_of(tile)] = value
        if final:
            for depth in range(8):
                patch_copy(row * 8 + depth).start()
        else:
            rate = rates(fine)
            send = jnp.where(fine, 1.0 / RESCALE, 1.0)
            for tile in range(TILES):
                field = [moved_ref[q, row, :, lanes_of(tile)] for q in range(SPEEDS)]
                balance = equilibria(field)
                for q in range(1, SPEEDS):
                    relaxed = field[q] + rate * (balance[q] - field[q])
                    eq_next[q, row, :, lanes_of(tile)] = balance[q]
                    neq_next[q, row, :, lanes_of(tile)] = send * (relaxed - balance[q])
        return carry

    def patch_copy(patch):
        return pltpu.make_async_copy(
            rows_ref.at[pl.ds(pl.multiple_of(patch * ROWS, 8), ROWS), :],
            moved_ref.at[targets[patch]],
            sems.at[patch],
        )

    lax.fori_loop(0, SPAN_PATCHES, move_row, 0)
    if final:

        def drain(patch, carry):
            patch_copy(patch).wait()
            return carry

        lax.fori_loop(0, SPAN_PATCHES * DEPTH_PATCHES, drain, 0)
    else:
        emit_halos(masks, eq_next, neq_next, 0, east_out, west_out, span_out, de_out, dw_out)


def unpack_kernel(patches, slots, received, out_ref, rows_ref, sems):
    def patch_copy(patch):
        return pltpu.make_async_copy(
            received.at[slots[patch]],
            rows_ref.at[pl.ds(pl.multiple_of(patch * ROWS, 8), ROWS), :],
            sems.at[patch],
        )

    def launch(patch, carry):
        patch_copy(patch).start()
        return carry

    def place(patch, carry):
        patch_copy(patch).wait()
        for first in range(0, SPEEDS, 8):
            count = min(8, SPEEDS - first)
            for tile in range(TILES):
                start = patch * ROWS + (first * TILES + tile)
                out_ref[patch, first : first + count, lanes_of(tile)] = rows_ref[
                    pl.ds(start, count, stride=TILES), :
                ]
        return carry

    lax.fori_loop(0, patches, launch, 0)
    lax.fori_loop(0, patches, place, 0)


def shape(*dims):
    return jax.ShapeDtypeStruct(dims, jnp.float32)


VMEM = pl.BlockSpec(memory_space=pltpu.VMEM)
SMEM = pl.BlockSpec(memory_space=pltpu.SMEM)
ANY = pl.BlockSpec(memory_space=pl.ANY)
PARAMS = pltpu.CompilerParams(vmem_limit_bytes=48 * 1024 * 1024)
FIELD = (SPEEDS, SPAN_PATCHES, DEPTH_PATCHES, CELLS)
FRAMED = (SPEEDS, SPAN_PATCHES + 2, DEPTH_PATCHES, CELLS)
SIDE = (len(X_SPEEDS), SPAN_PATCHES + 2, DEPTH_PATCHES, LANES)
ROW = (SPEEDS, DEPTH_PATCHES, CELLS)
HALOS = (
    shape(5, SPAN_PATCHES, DEPTH_PATCHES, LANES),
    shape(5, SPAN_PATCHES, DEPTH_PATCHES, LANES),
    shape(Y_PACKS, DEPTH_PATCHES, CELLS),
    shape(2, DEPTH_PATCHES, LANES),
    shape(2, DEPTH_PATCHES, LANES),
)


def scratch(dims):
    return pltpu.VMEM(dims, jnp.float32)


def exchange(east, west, span, diag_east, diag_west):
    blocks = lax.axis_size("blocks")
    cross = lax.axis_size("cross")

    def pairs(step_x, step_y):
        return [
            (b * cross + c, (b + step_x) * cross + (c + step_y) % cross)
            for b in range(blocks)
            for c in range(cross)
            if 0 <= b + step_x < blocks
        ]

    def send(value, step_x, step_y):
        return lax.ppermute(value, ("blocks", "cross"), pairs(step_x, step_y))

    def both(value, step_x):
        up = send(value, step_x, 1)
        return up, (up if cross == 2 else send(value, step_x, -1))

    north, south = both(span, 0)
    if cross == 2:
        de = send(diag_east, 1, 1)
        dw = send(diag_west, -1, 1)
    else:
        up, down = both(diag_east, 1)
        de = jnp.stack([up[0], down[1]])
        up, down = both(diag_west, -1)
        dw = jnp.stack([up[0], down[1]])
    return send(east, 1, 0), send(west, -1, 0), north, south, de, dw


def body(f_home, levels, plan):
    devices = lax.axis_size(("blocks", "cross"))
    here = lax.axis_index(("blocks", "cross"))
    patches = f_home.shape[0]
    capacity = (patches + devices - 1) // devices + 1
    block = lax.axis_index("blocks")
    ends = jnp.stack([block == 0, block == lax.axis_size("blocks") - 1]).astype(jnp.int32)
    level_rows = jnp.broadcast_to(
        levels.reshape(SPAN_PATCHES, DEPTH_PATCHES, 1), (SPAN_PATCHES, DEPTH_PATCHES, LANES)
    )

    outs = pl.pallas_call(
        open_kernel,
        out_shape=(shape(*FIELD),) + HALOS,
        in_specs=[VMEM, VMEM],
        out_specs=[VMEM] * 6,
        scratch_shapes=[scratch(FIELD), scratch(FIELD)],
        compiler_params=PARAMS,
        name="open",
    )(level_rows, f_home)
    field, halos = outs[0], exchange(*outs[1:])

    order = jnp.arange(patches, dtype=jnp.int32)
    owner = plan // patches
    earlier = (owner[:, None] == owner[None, :]) & (order[None, :] < order[:, None])
    targets = owner * capacity + jnp.sum(earlier.astype(jnp.int32), axis=1)

    whole_plan = lax.all_gather(plan, ("blocks", "cross"), tiled=True).reshape(devices, patches)
    mine = whole_plan // patches == here
    before = (order[:, None] < order[None, :]).astype(jnp.int32)
    rank = jnp.sum(mine[:, :, None].astype(jnp.int32) * before[None], axis=1)
    slot = jnp.arange(devices, dtype=jnp.int32)[:, None] * capacity + rank
    wanted = whole_plan[None] == (here * patches + order)[:, None, None]
    slots = jnp.sum(jnp.where(wanted, slot[None], 0), axis=(1, 2))

    common = [scratch(FRAMED), scratch(FRAMED), scratch(FIELD), scratch(SIDE), scratch(SIDE)]
    common += [scratch(ROW), scratch(ROW), scratch(ROW)]
    for _ in range(STEPS - 1):
        outs = pl.pallas_call(
            functools.partial(step_kernel, False),
            out_shape=(shape(*FIELD),) + HALOS,
            in_specs=[SMEM] + [VMEM] * 8,
            out_specs=[VMEM] * 6,
            scratch_shapes=common + [scratch(FIELD), scratch(FIELD)],
            compiler_params=PARAMS,
            name="step",
        )(ends, level_rows, field, *halos)
        field, halos = outs[0], exchange(*outs[1:])
    packed = pl.pallas_call(
        functools.partial(step_kernel, True),
        out_shape=shape(devices * capacity, ROWS, LANES),
        in_specs=[SMEM] + [VMEM] * 8 + [SMEM],
        out_specs=ANY,
        scratch_shapes=common
        + [scratch((patches * ROWS, LANES)), pltpu.SemaphoreType.DMA((patches,))],
        compiler_params=PARAMS,
        name="last",
    )(ends, level_rows, field, *halos, targets)
    received = lax.all_to_all(
        packed.reshape(devices, capacity * ROWS, LANES),
        ("blocks", "cross"),
        split_axis=0,
        concat_axis=0,
        tiled=True,
    ).reshape(devices * capacity, ROWS, LANES)
    return pl.pallas_call(
        functools.partial(unpack_kernel, patches),
        out_shape=shape(*f_home.shape),
        in_specs=[SMEM, ANY],
        out_specs=VMEM,
        scratch_shapes=[scratch((patches * ROWS, LANES)), pltpu.SemaphoreType.DMA((patches,))],
        compiler_params=PARAMS,
        name="unpack",
    )(slots, received)


def solution(mesh):
    in_specs = (P(("blocks", "cross"), None, None), P(("blocks", "cross")), P(("blocks", "cross")))
    out_specs = P(("blocks", "cross"), None, None)
    return jax.shard_map(body, mesh=mesh, in_specs=in_specs, out_specs=out_specs, check_vma=False)
```

```python
import functools

import jax
import jax.numpy as jnp
from jax import lax
from jax.experimental import pallas as pl
from jax.experimental.pallas import tpu as pltpu
from jax.sharding import PartitionSpec as P

SPAN_PATCHES = 4
DEPTH_PATCHES = 8
EDGE = 8
STEPS = 2
CELLS = 512
LANES = 128
TILES = CELLS // LANES
ROWS = 80

VELOCITIES = (
    (0, 0, 0),
    (1, 0, 0),
    (-1, 0, 0),
    (0, 1, 0),
    (0, -1, 0),
    (0, 0, 1),
    (0, 0, -1),
    (1, 1, 0),
    (-1, -1, 0),
    (1, -1, 0),
    (-1, 1, 0),
    (1, 0, 1),
    (-1, 0, -1),
    (1, 0, -1),
    (-1, 0, 1),
    (0, 1, 1),
    (0, -1, -1),
    (0, 1, -1),
    (0, -1, 1),
)
SPEEDS = 19
WEIGHTS = (1.0 / 3.0,) + (1.0 / 18.0,) * 6 + (1.0 / 36.0,) * 12
EAST = (1, 7, 9, 11, 13)
WEST = (2, 8, 10, 12, 14)
NORTH = (3, 7, 10, 15, 17)
SOUTH = (4, 8, 9, 16, 18)
X_SPEEDS = EAST + WEST
Y_SPEEDS = NORTH + SOUTH
Y_PACKS = 3
DIAG_EAST = ((7, SPAN_PATCHES - 1), (9, 0))
DIAG_WEST = ((10, SPAN_PATCHES - 1), (8, 0))
TAU_COARSE = 0.55
TAU_FINE = 2.0 * TAU_COARSE - 0.5
RESCALE = TAU_FINE / (2.0 * TAU_COARSE)
INFLOW = 0.08


def inflow_value(speed):
    along = VELOCITIES[speed][0] * INFLOW
    return WEIGHTS[speed] * (1.0 + 3.0 * along + 4.5 * along * along - 1.5 * INFLOW * INFLOW)


def lane_roll(tile, shift):
    shift %= LANES
    return tile if shift == 0 else pltpu.roll(tile, shift, 1)


def equilibria(field):
    density = functools.reduce(lambda a, b: a + b, field)
    inverse = 1.0 / density
    velocity = []
    for axis_id in range(3):
        forward = [field[q] for q in range(SPEEDS) if VELOCITIES[q][axis_id] == 1]
        backward = [field[q] for q in range(SPEEDS) if VELOCITIES[q][axis_id] == -1]
        terms = [a - b for a, b in zip(forward, backward)]
        velocity.append(functools.reduce(lambda a, b: a + b, terms) * inverse)
    common = 1.0 - 1.5 * (
        velocity[0] * velocity[0] + velocity[1] * velocity[1] + velocity[2] * velocity[2]
    )
    scaled = {weight: weight * density for weight in set(WEIGHTS)}
    balance = [scaled[WEIGHTS[0]] * common]
    for q in range(1, SPEEDS, 2):
        along = None
        for component, speed in zip(VELOCITIES[q], velocity):
            if component == 0:
                continue
            if along is None:
                along = speed if component == 1 else -speed
            else:
                along = along + speed if component == 1 else along - speed
        even = common + 4.5 * (along * along)
        odd = 3.0 * along
        balance.append(scaled[WEIGHTS[q]] * (even + odd))
        balance.append(scaled[WEIGHTS[q]] * (even - odd))
    return balance


class Masks:
    def __init__(self):
        lane = lax.broadcasted_iota(jnp.int32, (8, LANES), 1)
        self.low = lane < 64
        self.high = lane >= 64
        span = (lane // 8) % 8
        depth = lane % 8
        self.span = span
        self.span_first = span == 0
        self.span_last = span == 7
        self.depth_first = depth == 0
        self.depth_last = depth == 7

    def leaving(self, speed, tile):
        step_x, step_y, step_z = VELOCITIES[speed]
        across_x = None
        if step_x == 1 and tile == TILES - 1:
            across_x = self.high
        if step_x == -1 and tile == 0:
            across_x = self.low
        across_y = {0: None, 1: self.span_last, -1: self.span_first}[step_y]
        across_z = {0: None, 1: self.depth_last, -1: self.depth_first}[step_z]
        return across_x, across_y, across_z

    def leaving_any(self, speed, tile):
        parts = [mask for mask in self.leaving(speed, tile) if mask is not None]
        return functools.reduce(jnp.logical_or, parts) if parts else None

    def shifted(self, tiles, speed):
        step_x, step_y, step_z = VELOCITIES[speed]
        if step_z:
            edge = self.depth_first if step_z == 1 else self.depth_last
            tiles = [
                jnp.where(edge, lane_roll(v, -7 * step_z), lane_roll(v, step_z)) for v in tiles
            ]
        if step_y:
            edge = self.span_first if step_y == 1 else self.span_last
            tiles = [
                jnp.where(edge, lane_roll(v, -56 * step_y), lane_roll(v, 8 * step_y)) for v in tiles
            ]
        if step_x:
            halves = [lane_roll(v, 64) for v in tiles]
            if step_x == 1:
                tiles = [
                    jnp.where(self.low, halves[t - 1], halves[t]) for t in range(TILES)
                ]
            else:
                tiles = [
                    jnp.where(self.low, halves[t], halves[(t + 1) % TILES]) for t in range(TILES)
                ]
        return tiles


def lanes_of(tile):
    return pl.ds(tile * LANES, LANES)


def emit_halos(masks, eq, neq, east_ref, west_ref, span_ref):
    last = TILES - 1

    def east_pack(speed, row):
        e = eq[speed, row, :, lanes_of(last)]
        n = neq[speed, row, :, lanes_of(last)]
        return jnp.where(masks.low, lane_roll(e, 64), n)

    def west_pack(speed, row):
        e = eq[speed, row, :, lanes_of(0)]
        n = neq[speed, row, :, lanes_of(0)]
        return jnp.where(masks.low, e, lane_roll(n, 64))

    for column in range(5):
        for row in range(SPAN_PATCHES):
            east_ref[column * SPAN_PATCHES + row] = east_pack(EAST[column], row)
            west_ref[column * SPAN_PATCHES + row] = west_pack(WEST[column], row)
    for column, (speed, row) in enumerate(DIAG_EAST):
        span_ref[Y_PACKS * TILES + column] = east_pack(speed, row)
    for column, (speed, row) in enumerate(DIAG_WEST):
        span_ref[Y_PACKS * TILES + 2 + column] = west_pack(speed, row)
    for pack_id in range(Y_PACKS):
        for tile in range(TILES):
            packed = jnp.zeros((8, LANES), jnp.float32)
            for slot in range(4):
                index = pack_id * 4 + slot
                if index >= len(Y_SPEEDS):
                    continue
                north = index < 5
                row = SPAN_PATCHES - 1 if north else 0
                at = 7 if north else 0
                e = eq[Y_SPEEDS[index], row, :, lanes_of(tile)]
                n = neq[Y_SPEEDS[index], row, :, lanes_of(tile)]
                packed = jnp.where(
                    masks.span == 2 * slot, lane_roll(e, 8 * (2 * slot - at)), packed
                )
                packed = jnp.where(
                    masks.span == 2 * slot + 1, lane_roll(n, 8 * (2 * slot + 1 - at)), packed
                )
            span_ref[pack_id * TILES + tile] = packed


def take_halos(ends, span_eq, span_neq, side_eq, side_neq, east, west, north, south):
    for column, speed in enumerate(X_SPEEDS):
        rightward = column < 5
        closed = ends[0 if rightward else 1] == 1
        source, pairs = (east, DIAG_EAST) if rightward else (west, DIAG_WEST)
        first = column % 5 * SPAN_PATCHES
        parts = [(source[first + row], row + 1) for row in range(SPAN_PATCHES)]
        for entry, (diag_speed, row) in enumerate(pairs):
            if diag_speed == speed:
                parts.append((source[5 * SPAN_PATCHES + entry], 0 if row else SPAN_PATCHES + 1))
        for packed, row in parts:
            other = lane_roll(packed, 64)
            e, n = (other, packed) if rightward else (packed, other)
            side_eq[column, row] = jnp.where(closed, inflow_value(speed), e)
            side_neq[column, row] = jnp.where(closed, 0.0, n)
    for index in range(len(Y_SPEEDS)):
        from_south = index < 5
        source = north if from_south else south
        at = 7 if from_south else 0
        slot = index % 4
        for tile in range(TILES):
            packed = source[index // 4 * TILES + tile]
            span_eq[index, :, lanes_of(tile)] = lane_roll(packed, 8 * (at - 2 * slot))
            span_neq[index, :, lanes_of(tile)] = lane_roll(packed, 8 * (at - 2 * slot - 1))


def rates(fine):
    return jnp.where(fine, 1.0 / TAU_FINE, 1.0 / TAU_COARSE)


def relax(masks, field, fine, row, tile, relaxed_ref, eq, neq):
    balance = equilibria(field)
    rate = rates(fine)
    send = jnp.where(fine, 1.0 / RESCALE, 1.0)
    for q in range(SPEEDS):
        relaxed = field[q] + rate * (balance[q] - field[q])
        relaxed_ref[q, row, :, lanes_of(tile)] = relaxed
        if q:
            eq[q, row, :, lanes_of(tile)] = balance[q]
            neq[q, row, :, lanes_of(tile)] = send * (relaxed - balance[q])


def open_kernel(level_ref, field_ref, relaxed_ref, eq, neq, east, west, span):
    masks = Masks()

    def row_step(row, carry):
        fine = level_ref[row] == 1
        for tile in range(TILES):
            field = [field_ref[pl.ds(row * 8, 8), q, lanes_of(tile)] for q in range(SPEEDS)]
            relax(masks, field, fine, row, tile, relaxed_ref, eq, neq)
        return carry

    lax.fori_loop(0, SPAN_PATCHES, row_step, 0)
    emit_halos(masks, eq, neq, east, west, span)


def step_kernel(final, *refs):
    ends, level_ref, relaxed_ref, eq, neq, east, west, north, south = refs[:9]
    if final:
        targets, _, moved_ref = refs[9:12]
        span_eq, span_neq, side_eq, side_neq, ghost, fresh, again, rows_ref, sems = refs[12:]
    else:
        relaxed_next, eq_next, neq_next, east_out, west_out, span_out = refs[9:15]
        span_eq, span_neq, side_eq, side_neq, ghost, fresh, again = refs[15:]
    masks = Masks()
    take_halos(ends, span_eq, span_neq, side_eq, side_neq, east, west, north, south)

    def move_row(row, carry):
        fine = level_ref[row] == 1
        scale = jnp.where(fine, RESCALE, 1.0)
        for q in range(SPEEDS):
            _, step_y, step_z = VELOCITIES[q]
            tiles = []
            for tile in range(TILES):
                value = relaxed_ref[q, row, :, lanes_of(tile)]
                across_x, across_y, across_z = masks.leaving(q, tile)

                def source(inner, side, outer, step_y):
                    at = row - step_y
                    if step_y:
                        beyond = outer[Y_SPEEDS.index(q), :, lanes_of(tile)]
                        inside = inner[q, jnp.clip(at, 0, SPAN_PATCHES - 1), :, lanes_of(tile)]
                        edge = 0 if step_y == 1 else SPAN_PATCHES - 1
                        picked = jnp.where(row == edge, beyond, inside)
                    else:
                        picked = inner[q, at, :, lanes_of(tile)]
                    if across_x is not None:
                        picked = jnp.where(across_x, side[X_SPEEDS.index(q), at + 1], picked)
                    return picked

                crossing = masks.leaving_any(q, tile)
                if crossing is not None:
                    pair = []
                    for group in ((eq, side_eq, span_eq), (neq, side_neq, span_neq)):
                        picked = source(*group, 0)
                        if across_y is not None:
                            picked = jnp.where(across_y, source(*group, step_y), picked)
                        if across_z is not None:
                            turned = pltpu.roll(picked, step_z % DEPTH_PATCHES, 0)
                            picked = jnp.where(across_z, turned, picked)
                        pair.append(picked)
                    value = jnp.where(crossing, pair[0] + scale * pair[1], value)
                    ghost[q, :, lanes_of(tile)] = value
                tiles.append(value)
            for tile, value in enumerate(masks.shifted(tiles, q)):
                fresh[q, :, lanes_of(tile)] = value
        for tile in range(TILES):
            field = [fresh[q, :, lanes_of(tile)] for q in range(SPEEDS)]
            balance = equilibria(field)
            for q in range(SPEEDS):
                again[q, :, lanes_of(tile)] = field[q] + (1.0 / TAU_FINE) * (balance[q] - field[q])
        for q in range(SPEEDS):
            tiles = []
            for tile in range(TILES):
                value = again[q, :, lanes_of(tile)]
                crossing = masks.leaving_any(q, tile)
                if crossing is not None:
                    value = jnp.where(crossing, ghost[q, :, lanes_of(tile)], value)
                tiles.append(value)
            for tile, value in enumerate(masks.shifted(tiles, q)):
                value = jnp.where(fine, value, fresh[q, :, lanes_of(tile)])
                if final:
                    start = row * (8 * ROWS) + (q * TILES + tile)
                    rows_ref[pl.ds(start, 8, stride=ROWS), :] = value
                else:
                    fresh[q, :, lanes_of(tile)] = value
        if final:
            for depth in range(8):
                patch_copy(row * 8 + depth).start()
        else:
            for tile in range(TILES):
                field = [fresh[q, :, lanes_of(tile)] for q in range(SPEEDS)]
                relax(masks, field, fine, row, tile, relaxed_next, eq_next, neq_next)
        return carry

    def patch_copy(patch):
        return pltpu.make_async_copy(
            rows_ref.at[pl.ds(pl.multiple_of(patch * ROWS, 8), ROWS), :],
            moved_ref.at[targets[patch]],
            sems.at[patch],
        )

    lax.fori_loop(0, SPAN_PATCHES, move_row, 0)
    if final:

        def drain(patch, carry):
            patch_copy(patch).wait()
            return carry

        lax.fori_loop(0, SPAN_PATCHES * DEPTH_PATCHES, drain, 0)
    else:
        emit_halos(masks, eq_next, neq_next, east_out, west_out, span_out)


def unpack_kernel(patches, slots, received, out_ref, rows_ref, sems):
    def patch_copy(patch):
        return pltpu.make_async_copy(
            received.at[slots[patch]],
            rows_ref.at[pl.ds(pl.multiple_of(patch * ROWS, 8), ROWS), :],
            sems.at[patch],
        )

    def launch(patch, carry):
        patch_copy(patch).start()
        return carry

    def place(patch, carry):
        patch_copy(patch).wait()
        for first in range(0, SPEEDS, 8):
            count = min(8, SPEEDS - first)
            for tile in range(TILES):
                start = patch * ROWS + (first * TILES + tile)
                out_ref[patch, first : first + count, lanes_of(tile)] = rows_ref[
                    pl.ds(start, count, stride=TILES), :
                ]
        return carry

    lax.fori_loop(0, patches, launch, 0)
    lax.fori_loop(0, patches, place, 0)


def shape(*dims):
    return jax.ShapeDtypeStruct(dims, jnp.float32)


VMEM = pl.BlockSpec(memory_space=pltpu.VMEM)
SMEM = pl.BlockSpec(memory_space=pltpu.SMEM)
ANY = pl.BlockSpec(memory_space=pl.ANY)
PARAMS = pltpu.CompilerParams(vmem_limit_bytes=16 * 1024 * 1024)
FIELD = (SPEEDS, SPAN_PATCHES, DEPTH_PATCHES, CELLS)
SIDE = (len(X_SPEEDS), SPAN_PATCHES + 2, DEPTH_PATCHES, LANES)
ROW = (SPEEDS, DEPTH_PATCHES, CELLS)
SPAN = (len(X_SPEEDS), DEPTH_PATCHES, CELLS)
HANDED = (
    shape(*FIELD),
    shape(*FIELD),
    shape(*FIELD),
    shape(5 * SPAN_PATCHES, DEPTH_PATCHES, LANES),
    shape(5 * SPAN_PATCHES, DEPTH_PATCHES, LANES),
    shape(Y_PACKS * TILES + 4, DEPTH_PATCHES, LANES),
)


def scratch(dims):
    return pltpu.VMEM(dims, jnp.float32)


def exchange(east, west, span):
    blocks = lax.axis_size("blocks")
    cross = lax.axis_size("cross")

    def send_span(step):
        return lax.ppermute(span, "cross", [(c, (c + step) % cross) for c in range(cross)])

    def send_flow(value, corner, step):
        whole = jnp.concatenate([value, corner])
        pairs = [(b, b + step) for b in range(blocks) if 0 <= b + step < blocks]
        return lax.ppermute(whole, "blocks", pairs)

    north = send_span(1)
    south = north if cross == 2 else send_span(-1)
    first = Y_PACKS * TILES
    corners = [north[first : first + 1], south[first + 1 : first + 2]]
    corners += [north[first + 2 : first + 3], south[first + 3 : first + 4]]
    if cross == 2:
        corner_east, corner_west = north[first : first + 2], north[first + 2 : first + 4]
    else:
        corner_east, corner_west = jnp.concatenate(corners[:2]), jnp.concatenate(corners[2:])
    return send_flow(east, corner_east, 1), send_flow(west, corner_west, -1), north, south


def body(f_home, levels, plan):
    devices = lax.axis_size(("blocks", "cross"))
    here = lax.axis_index(("blocks", "cross"))
    patches = f_home.shape[0]
    capacity = (patches + devices - 1) // devices + 1
    block = lax.axis_index("blocks")
    ends = jnp.stack([block == 0, block == lax.axis_size("blocks") - 1]).astype(jnp.int32)
    level_rows = jnp.broadcast_to(
        levels.reshape(SPAN_PATCHES, DEPTH_PATCHES, 1), (SPAN_PATCHES, DEPTH_PATCHES, LANES)
    )

    order = jnp.arange(patches, dtype=jnp.int32)
    owner = plan // patches
    earlier = (owner[:, None] == owner[None, :]) & (order[None, :] < order[:, None])
    targets = owner * capacity + jnp.sum(earlier.astype(jnp.int32), axis=1)
    table_order = jnp.arange(devices * capacity, dtype=jnp.int32)
    table = jnp.sum(
        jnp.where(targets[None, :] == table_order[:, None], plan[None, :] % patches + 1, 0), axis=1
    )
    table = lax.all_to_all(
        table.reshape(devices, capacity), ("blocks", "cross"), 0, 0, tiled=True
    ).reshape(devices * capacity)
    slots = jnp.sum(
        jnp.where(table[None, :] == order[:, None] + 1, table_order[None, :], 0), axis=1
    )

    outs = pl.pallas_call(
        open_kernel,
        out_shape=HANDED,
        in_specs=[VMEM, VMEM],
        out_specs=[VMEM] * 6,
        compiler_params=PARAMS,
        name="open",
    )(level_rows, f_home)
    common = [scratch(SPAN), scratch(SPAN), scratch(SIDE), scratch(SIDE)]
    common += [scratch(ROW), scratch(ROW), scratch(ROW)]
    for _ in range(STEPS - 1):
        outs = pl.pallas_call(
            functools.partial(step_kernel, False),
            out_shape=HANDED,
            in_specs=[SMEM] + [VMEM] * 8,
            out_specs=[VMEM] * 6,
            scratch_shapes=common,
            compiler_params=PARAMS,
            name="step",
        )(ends, level_rows, *outs[:3], *exchange(*outs[3:]))
    packed = pl.pallas_call(
        functools.partial(step_kernel, True),
        out_shape=shape(devices * capacity, ROWS, LANES),
        in_specs=[SMEM] + [VMEM] * 8 + [SMEM, SMEM],
        out_specs=ANY,
        scratch_shapes=common
        + [scratch((patches * ROWS, LANES)), pltpu.SemaphoreType.DMA((patches,))],
        compiler_params=PARAMS,
        name="last",
    )(ends, level_rows, *outs[:3], *exchange(*outs[3:]), targets, slots)
    received = lax.all_to_all(
        packed.reshape(devices, capacity * ROWS, LANES),
        ("blocks", "cross"),
        split_axis=0,
        concat_axis=0,
        tiled=True,
    ).reshape(devices * capacity, ROWS, LANES)
    return pl.pallas_call(
        functools.partial(unpack_kernel, patches),
        out_shape=shape(*f_home.shape),
        in_specs=[SMEM, ANY],
        out_specs=VMEM,
        scratch_shapes=[scratch((patches * ROWS, LANES)), pltpu.SemaphoreType.DMA((patches,))],
        compiler_params=PARAMS,
        name="unpack",
    )(slots, received)


def solution(mesh):
    in_specs = (P(("blocks", "cross"), None, None), P(("blocks", "cross")), P(("blocks", "cross")))
    out_specs = P(("blocks", "cross"), None, None)
    return jax.shard_map(body, mesh=mesh, in_specs=in_specs, out_specs=out_specs, check_vma=False)
```

```python
import functools

import jax
import jax.numpy as jnp
from jax import lax
from jax.experimental import pallas as pl
from jax.experimental.pallas import tpu as pltpu
from jax.sharding import PartitionSpec as P

SPAN_PATCHES = 4
DEPTH_PATCHES = 8
EDGE = 8
STEPS = 2
CELLS = 512
LANES = 128
TILES = CELLS // LANES
ROWS = 80

VELOCITIES = (
    (0, 0, 0),
    (1, 0, 0),
    (-1, 0, 0),
    (0, 1, 0),
    (0, -1, 0),
    (0, 0, 1),
    (0, 0, -1),
    (1, 1, 0),
    (-1, -1, 0),
    (1, -1, 0),
    (-1, 1, 0),
    (1, 0, 1),
    (-1, 0, -1),
    (1, 0, -1),
    (-1, 0, 1),
    (0, 1, 1),
    (0, -1, -1),
    (0, 1, -1),
    (0, -1, 1),
)
SPEEDS = 19
WEIGHTS = (1.0 / 3.0,) + (1.0 / 18.0,) * 6 + (1.0 / 36.0,) * 12
EAST = (1, 7, 9, 11, 13)
WEST = (2, 8, 10, 12, 14)
NORTH = (3, 7, 10, 15, 17)
SOUTH = (4, 8, 9, 16, 18)
X_SPEEDS = EAST + WEST
Y_SPEEDS = NORTH + SOUTH
Y_PACKS = 3
DIAG_EAST = ((7, SPAN_PATCHES - 1), (9, 0))
DIAG_WEST = ((10, SPAN_PATCHES - 1), (8, 0))
TAU_COARSE = 0.55
TAU_FINE = 2.0 * TAU_COARSE - 0.5
RESCALE = TAU_FINE / (2.0 * TAU_COARSE)
INFLOW = 0.08


def inflow_value(speed):
    along = VELOCITIES[speed][0] * INFLOW
    return WEIGHTS[speed] * (1.0 + 3.0 * along + 4.5 * along * along - 1.5 * INFLOW * INFLOW)


def lane_roll(tile, shift):
    shift %= LANES
    return tile if shift == 0 else pltpu.roll(tile, shift, 1)


def equilibria(field):
    density = functools.reduce(lambda a, b: a + b, field)
    inverse = 1.0 / density
    velocity = []
    for axis_id in range(3):
        forward = [field[q] for q in range(SPEEDS) if VELOCITIES[q][axis_id] == 1]
        backward = [field[q] for q in range(SPEEDS) if VELOCITIES[q][axis_id] == -1]
        terms = [a - b for a, b in zip(forward, backward)]
        velocity.append(functools.reduce(lambda a, b: a + b, terms) * inverse)
    common = 1.0 - 1.5 * (
        velocity[0] * velocity[0] + velocity[1] * velocity[1] + velocity[2] * velocity[2]
    )
    scaled = {weight: weight * density for weight in set(WEIGHTS)}
    balance = [scaled[WEIGHTS[0]] * common]
    for q in range(1, SPEEDS, 2):
        along = None
        for component, speed in zip(VELOCITIES[q], velocity):
            if component == 0:
                continue
            if along is None:
                along = speed if component == 1 else -speed
            else:
                along = along + speed if component == 1 else along - speed
        even = common + 4.5 * (along * along)
        odd = 3.0 * along
        balance.append(scaled[WEIGHTS[q]] * (even + odd))
        balance.append(scaled[WEIGHTS[q]] * (even - odd))
    return balance


class Masks:
    def __init__(self):
        lane = lax.broadcasted_iota(jnp.int32, (8, LANES), 1)
        self.low = lane < 64
        self.high = lane >= 64
        span = (lane // 8) % 8
        depth = lane % 8
        self.span = span
        self.span_first = span == 0
        self.span_last = span == 7
        self.depth_first = depth == 0
        self.depth_last = depth == 7

    def leaving(self, speed, tile):
        step_x, step_y, step_z = VELOCITIES[speed]
        across_x = None
        if step_x == 1 and tile == TILES - 1:
            across_x = self.high
        if step_x == -1 and tile == 0:
            across_x = self.low
        across_y = {0: None, 1: self.span_last, -1: self.span_first}[step_y]
        across_z = {0: None, 1: self.depth_last, -1: self.depth_first}[step_z]
        return across_x, across_y, across_z

    def leaving_any(self, speed, tile):
        parts = [mask for mask in self.leaving(speed, tile) if mask is not None]
        return functools.reduce(jnp.logical_or, parts) if parts else None

    def shifted(self, tiles, speed):
        step_x, step_y, step_z = VELOCITIES[speed]
        if step_z:
            edge = self.depth_first if step_z == 1 else self.depth_last
            tiles = [
                jnp.where(edge, lane_roll(v, -7 * step_z), lane_roll(v, step_z)) for v in tiles
            ]
        if step_y:
            edge = self.span_first if step_y == 1 else self.span_last
            tiles = [
                jnp.where(edge, lane_roll(v, -56 * step_y), lane_roll(v, 8 * step_y)) for v in tiles
            ]
        if step_x:
            halves = [lane_roll(v, 64) for v in tiles]
            if step_x == 1:
                tiles = [
                    jnp.where(self.low, halves[t - 1], halves[t]) for t in range(TILES)
                ]
            else:
                tiles = [
                    jnp.where(self.low, halves[t], halves[(t + 1) % TILES]) for t in range(TILES)
                ]
        return tiles


def lanes_of(tile):
    return pl.ds(tile * LANES, LANES)


def emit_halos(masks, eq, neq, east_ref, west_ref, span_ref):
    last = TILES - 1

    def east_pack(speed, row):
        e = eq[speed, row, :, lanes_of(last)]
        n = neq[speed, row, :, lanes_of(last)]
        return jnp.where(masks.low, lane_roll(e, 64), n)

    def west_pack(speed, row):
        e = eq[speed, row, :, lanes_of(0)]
        n = neq[speed, row, :, lanes_of(0)]
        return jnp.where(masks.low, e, lane_roll(n, 64))

    for column in range(5):
        for row in range(SPAN_PATCHES):
            east_ref[column * SPAN_PATCHES + row] = east_pack(EAST[column], row)
            west_ref[column * SPAN_PATCHES + row] = west_pack(WEST[column], row)
    for column, (speed, row) in enumerate(DIAG_EAST):
        span_ref[Y_PACKS * TILES + column] = east_pack(speed, row)
    for column, (speed, row) in enumerate(DIAG_WEST):
        span_ref[Y_PACKS * TILES + 2 + column] = west_pack(speed, row)
    for pack_id in range(Y_PACKS):
        for tile in range(TILES):
            packed = jnp.zeros((8, LANES), jnp.float32)
            for slot in range(4):
                index = pack_id * 4 + slot
                if index >= len(Y_SPEEDS):
                    continue
                north = index < 5
                row = SPAN_PATCHES - 1 if north else 0
                at = 7 if north else 0
                e = eq[Y_SPEEDS[index], row, :, lanes_of(tile)]
                n = neq[Y_SPEEDS[index], row, :, lanes_of(tile)]
                packed = jnp.where(
                    masks.span == 2 * slot, lane_roll(e, 8 * (2 * slot - at)), packed
                )
                packed = jnp.where(
                    masks.span == 2 * slot + 1, lane_roll(n, 8 * (2 * slot + 1 - at)), packed
                )
            span_ref[pack_id * TILES + tile] = packed


def take_halos(ends, span_eq, span_neq, side_eq, side_neq, east, west, north, south):
    for column, speed in enumerate(X_SPEEDS):
        rightward = column < 5
        closed = ends[0 if rightward else 1] == 1
        source, pairs = (east, DIAG_EAST) if rightward else (west, DIAG_WEST)
        first = column % 5 * SPAN_PATCHES
        parts = [(source[first + row], row + 1) for row in range(SPAN_PATCHES)]
        for entry, (diag_speed, row) in enumerate(pairs):
            if diag_speed == speed:
                parts.append((source[5 * SPAN_PATCHES + entry], 0 if row else SPAN_PATCHES + 1))
        for packed, row in parts:
            other = lane_roll(packed, 64)
            e, n = (other, packed) if rightward else (packed, other)
            side_eq[column, row] = jnp.where(closed, inflow_value(speed), e)
            side_neq[column, row] = jnp.where(closed, 0.0, n)
    for index in range(len(Y_SPEEDS)):
        from_south = index < 5
        source = north if from_south else south
        at = 7 if from_south else 0
        slot = index % 4
        for tile in range(TILES):
            packed = source[index // 4 * TILES + tile]
            span_eq[index, :, lanes_of(tile)] = lane_roll(packed, 8 * (at - 2 * slot))
            span_neq[index, :, lanes_of(tile)] = lane_roll(packed, 8 * (at - 2 * slot - 1))


def rates(fine):
    return jnp.where(fine, 1.0 / TAU_FINE, 1.0 / TAU_COARSE)


def relax(field, fine, row, tile, relaxed_ref, eq, neq):
    balance = equilibria(field)
    rate = rates(fine)
    send = jnp.where(fine, 1.0 / RESCALE, 1.0)
    for q in range(SPEEDS):
        relaxed = field[q] + rate * (balance[q] - field[q])
        if relaxed_ref is not None:
            relaxed_ref[q, row, :, lanes_of(tile)] = relaxed
        if q:
            eq[q, row, :, lanes_of(tile)] = balance[q]
            neq[q, row, :, lanes_of(tile)] = send * (relaxed - balance[q])


def open_kernel(level_ref, field_ref, moved_ref, east, west, span, eq, neq):
    masks = Masks()

    def row_step(row, carry):
        fine = level_ref[row] == 1
        for tile in range(TILES):
            field = [field_ref[pl.ds(row * 8, 8), q, lanes_of(tile)] for q in range(SPEEDS)]
            for q in range(SPEEDS):
                moved_ref[q, row, :, lanes_of(tile)] = field[q]
            relax(field, fine, row, tile, None, eq, neq)
        return carry

    lax.fori_loop(0, SPAN_PATCHES, row_step, 0)
    emit_halos(masks, eq, neq, east, west, span)


def step_kernel(final, *refs):
    ends, level_ref, field_ref, east, west, north, south = refs[:7]
    if final:
        targets, _, moved_ref = refs[7:10]
        held, (rows_ref, sems) = refs[10:20], refs[20:]
    else:
        moved_ref, east_out, west_out, span_out = refs[7:11]
        held, (eq_next, neq_next) = refs[11:21], refs[21:]
    relaxed_ref, eq, neq, span_eq, span_neq, side_eq, side_neq, ghost, fresh, again = held
    masks = Masks()
    take_halos(ends, span_eq, span_neq, side_eq, side_neq, east, west, north, south)

    def collide_row(row, carry):
        fine = level_ref[row] == 1
        for tile in range(TILES):
            field = [field_ref[q, row, :, lanes_of(tile)] for q in range(SPEEDS)]
            relax(field, fine, row, tile, relaxed_ref, eq, neq)
        return carry

    lax.fori_loop(0, SPAN_PATCHES, collide_row, 0)

    def move_row(row, carry):
        fine = level_ref[row] == 1
        scale = jnp.where(fine, RESCALE, 1.0)
        for q in range(SPEEDS):
            _, step_y, step_z = VELOCITIES[q]
            tiles = []
            for tile in range(TILES):
                value = relaxed_ref[q, row, :, lanes_of(tile)]
                across_x, across_y, across_z = masks.leaving(q, tile)

                def source(inner, side, outer, step_y):
                    at = row - step_y
                    if step_y:
                        beyond = outer[Y_SPEEDS.index(q), :, lanes_of(tile)]
                        inside = inner[q, jnp.clip(at, 0, SPAN_PATCHES - 1), :, lanes_of(tile)]
                        edge = 0 if step_y == 1 else SPAN_PATCHES - 1
                        picked = jnp.where(row == edge, beyond, inside)
                    else:
                        picked = inner[q, at, :, lanes_of(tile)]
                    if across_x is not None:
                        picked = jnp.where(across_x, side[X_SPEEDS.index(q), at + 1], picked)
                    return picked

                crossing = masks.leaving_any(q, tile)
                if crossing is not None:
                    pair = []
                    for group in ((eq, side_eq, span_eq), (neq, side_neq, span_neq)):
                        picked = source(*group, 0)
                        if across_y is not None:
                            picked = jnp.where(across_y, source(*group, step_y), picked)
                        if across_z is not None:
                            turned = pltpu.roll(picked, step_z % DEPTH_PATCHES, 0)
                            picked = jnp.where(across_z, turned, picked)
                        pair.append(picked)
                    value = jnp.where(crossing, pair[0] + scale * pair[1], value)
                    ghost[q, :, lanes_of(tile)] = value
                tiles.append(value)
            for tile, value in enumerate(masks.shifted(tiles, q)):
                fresh[q, :, lanes_of(tile)] = value
        for tile in range(TILES):
            field = [fresh[q, :, lanes_of(tile)] for q in range(SPEEDS)]
            balance = equilibria(field)
            for q in range(SPEEDS):
                again[q, :, lanes_of(tile)] = field[q] + (1.0 / TAU_FINE) * (balance[q] - field[q])
        for q in range(SPEEDS):
            tiles = []
            for tile in range(TILES):
                value = again[q, :, lanes_of(tile)]
                crossing = masks.leaving_any(q, tile)
                if crossing is not None:
                    value = jnp.where(crossing, ghost[q, :, lanes_of(tile)], value)
                tiles.append(value)
            for tile, value in enumerate(masks.shifted(tiles, q)):
                value = jnp.where(fine, value, fresh[q, :, lanes_of(tile)])
                if final:
                    start = row * (8 * ROWS) + (q * TILES + tile)
                    rows_ref[pl.ds(start, 8, stride=ROWS), :] = value
                else:
                    moved_ref[q, row, :, lanes_of(tile)] = value
        if final:
            for depth in range(8):
                patch_copy(row * 8 + depth).start()
        else:
            for tile in range(TILES):
                field = [moved_ref[q, row, :, lanes_of(tile)] for q in range(SPEEDS)]
                relax(field, fine, row, tile, None, eq_next, neq_next)
        return carry

    def patch_copy(patch):
        return pltpu.make_async_copy(
            rows_ref.at[pl.ds(pl.multiple_of(patch * ROWS, 8), ROWS), :],
            moved_ref.at[targets[patch]],
            sems.at[patch],
        )

    lax.fori_loop(0, SPAN_PATCHES, move_row, 0)
    if final:

        def drain(patch, carry):
            patch_copy(patch).wait()
            return carry

        lax.fori_loop(0, SPAN_PATCHES * DEPTH_PATCHES, drain, 0)
    else:
        emit_halos(masks, eq_next, neq_next, east_out, west_out, span_out)


def unpack_kernel(patches, slots, received, out_ref, rows_ref, placed_ref, sems, out_sems):
    def patch_copy(patch):
        return pltpu.make_async_copy(
            received.at[slots[patch]],
            rows_ref.at[pl.ds(pl.multiple_of(patch * ROWS, 8), ROWS), :],
            sems.at[patch],
        )

    def out_copy(patch):
        return pltpu.make_async_copy(
            placed_ref.at[patch], out_ref.at[patch], out_sems.at[patch]
        )

    def launch(patch, carry):
        patch_copy(patch).start()
        return carry

    def place(patch, carry):
        patch_copy(patch).wait()
        for first in range(0, SPEEDS, 8):
            count = min(8, SPEEDS - first)
            for tile in range(TILES):
                start = patch * ROWS + (first * TILES + tile)
                placed_ref[patch, first : first + count, lanes_of(tile)] = rows_ref[
                    pl.ds(start, count, stride=TILES), :
                ]
        out_copy(patch).start()
        return carry

    lax.fori_loop(0, patches, launch, 0)
    def drain(patch, carry):
        out_copy(patch).wait()
        return carry

    lax.fori_loop(0, patches, place, 0)
    lax.fori_loop(0, patches, drain, 0)


def shape(*dims):
    return jax.ShapeDtypeStruct(dims, jnp.float32)


VMEM = pl.BlockSpec(memory_space=pltpu.VMEM)
SMEM = pl.BlockSpec(memory_space=pltpu.SMEM)
ANY = pl.BlockSpec(memory_space=pl.ANY)
PARAMS = pltpu.CompilerParams(vmem_limit_bytes=16 * 1024 * 1024)
FIELD = (SPEEDS, SPAN_PATCHES, DEPTH_PATCHES, CELLS)
SIDE = (len(X_SPEEDS), SPAN_PATCHES + 2, DEPTH_PATCHES, LANES)
ROW = (SPEEDS, DEPTH_PATCHES, CELLS)
SPAN = (len(X_SPEEDS), DEPTH_PATCHES, CELLS)
HANDED = (
    shape(*FIELD),
    shape(5 * SPAN_PATCHES, DEPTH_PATCHES, LANES),
    shape(5 * SPAN_PATCHES, DEPTH_PATCHES, LANES),
    shape(Y_PACKS * TILES + 4, DEPTH_PATCHES, LANES),
)


def scratch(dims):
    return pltpu.VMEM(dims, jnp.float32)


def exchange(east, west, span):
    blocks = lax.axis_size("blocks")
    cross = lax.axis_size("cross")

    def send_span(step):
        return lax.ppermute(span, "cross", [(c, (c + step) % cross) for c in range(cross)])

    def send_flow(value, corner, step):
        whole = jnp.concatenate([value, corner])
        pairs = [(b, b + step) for b in range(blocks) if 0 <= b + step < blocks]
        return lax.ppermute(whole, "blocks", pairs)

    north = send_span(1)
    south = north if cross == 2 else send_span(-1)
    first = Y_PACKS * TILES
    corners = [north[first : first + 1], south[first + 1 : first + 2]]
    corners += [north[first + 2 : first + 3], south[first + 3 : first + 4]]
    if cross == 2:
        corner_east, corner_west = north[first : first + 2], north[first + 2 : first + 4]
    else:
        corner_east, corner_west = jnp.concatenate(corners[:2]), jnp.concatenate(corners[2:])
    return send_flow(east, corner_east, 1), send_flow(west, corner_west, -1), north, south


def body(f_home, levels, plan):
    devices = lax.axis_size(("blocks", "cross"))
    here = lax.axis_index(("blocks", "cross"))
    patches = f_home.shape[0]
    capacity = (patches + devices - 1) // devices + 1
    block = lax.axis_index("blocks")
    ends = jnp.stack([block == 0, block == lax.axis_size("blocks") - 1]).astype(jnp.int32)
    level_rows = jnp.broadcast_to(
        levels.reshape(SPAN_PATCHES, DEPTH_PATCHES, 1), (SPAN_PATCHES, DEPTH_PATCHES, LANES)
    )

    order = jnp.arange(patches, dtype=jnp.int32)
    owner = plan // patches
    earlier = (owner[:, None] == owner[None, :]) & (order[None, :] < order[:, None])
    targets = owner * capacity + jnp.sum(earlier.astype(jnp.int32), axis=1)
    table_order = jnp.arange(devices * capacity, dtype=jnp.int32)
    table = jnp.sum(
        jnp.where(targets[None, :] == table_order[:, None], plan[None, :] % patches + 1, 0), axis=1
    )
    table = lax.all_to_all(
        table.reshape(devices, capacity), ("blocks", "cross"), 0, 0, tiled=True
    ).reshape(devices * capacity)
    slots = jnp.sum(
        jnp.where(table[None, :] == order[:, None] + 1, table_order[None, :], 0), axis=1
    )

    outs = pl.pallas_call(
        open_kernel,
        out_shape=HANDED,
        in_specs=[VMEM, VMEM],
        out_specs=[VMEM] * 4,
        scratch_shapes=[scratch(FIELD), scratch(FIELD)],
        compiler_params=PARAMS,
        name="open",
    )(level_rows, f_home)
    common = [scratch(FIELD), scratch(FIELD), scratch(FIELD)]
    common += [scratch(SPAN), scratch(SPAN), scratch(SIDE), scratch(SIDE)]
    common += [scratch(ROW), scratch(ROW), scratch(ROW)]
    for _ in range(STEPS - 1):
        outs = pl.pallas_call(
            functools.partial(step_kernel, False),
            out_shape=HANDED,
            in_specs=[SMEM] + [VMEM] * 6,
            out_specs=[VMEM] * 4,
            scratch_shapes=common + [scratch(FIELD), scratch(FIELD)],
            compiler_params=PARAMS,
            name="step",
        )(ends, level_rows, outs[0], *exchange(*outs[1:]))
    packed = pl.pallas_call(
        functools.partial(step_kernel, True),
        out_shape=shape(devices * capacity, ROWS, LANES),
        in_specs=[SMEM] + [VMEM] * 6 + [SMEM, SMEM],
        out_specs=ANY,
        scratch_shapes=common
        + [scratch((patches * ROWS, LANES)), pltpu.SemaphoreType.DMA((patches,))],
        compiler_params=PARAMS,
        name="last",
    )(ends, level_rows, outs[0], *exchange(*outs[1:]), targets, slots)
    received = lax.all_to_all(
        packed.reshape(devices, capacity * ROWS, LANES),
        ("blocks", "cross"),
        split_axis=0,
        concat_axis=0,
        tiled=True,
    ).reshape(devices * capacity, ROWS, LANES)
    return pl.pallas_call(
        functools.partial(unpack_kernel, patches),
        out_shape=shape(*f_home.shape),
        in_specs=[SMEM, ANY],
        out_specs=pl.BlockSpec(memory_space=pltpu.HBM),
        scratch_shapes=[
            scratch((patches * ROWS, LANES)),
            scratch(f_home.shape),
            pltpu.SemaphoreType.DMA((patches,)),
            pltpu.SemaphoreType.DMA((patches,)),
        ],
        compiler_params=PARAMS,
        name="unpack",
    )(slots, received)


def solution(mesh):
    in_specs = (P(("blocks", "cross"), None, None), P(("blocks", "cross")), P(("blocks", "cross")))
    out_specs = P(("blocks", "cross"), None, None)
    return jax.shard_map(body, mesh=mesh, in_specs=in_specs, out_specs=out_specs, check_vma=False)
```
